256 devices in a mesh: strip: 256 (over x, z, y, core).
Axes of the slice: x: 4, y: 4, z: 8, core: 2. Of those that a mesh axis runs over, the one named last changes fastest.
Arguments:
- features: bfloat16 [64, 8192, 1024], P(None, 'strip'), may hold values from -6 to 6
- row_kernel: bfloat16 [8, 8, 8, 129], replicated, may hold values from -0.1875 to 0.1875
- mix_weight: bfloat16 [64, 64], replicated, may hold values from -0.75 to 0.75
- channel_bias: float32 [64], replicated, may hold values from -3 to 3
Outputs:
- layer_out: bfloat16 [64, 8192, 1024], P(None, 'strip')
The draws below stay inside these ranges and needn't reach their ends.
All inputs are finite; a program needn't handle non-finite values.
Results may differ from the reference program's by a relative error of at most 0.001.
Values may be sent and summed in bfloat16 or wider, within the bound.
No kernel may reach another device: no remote copies, remote signals or barrier semaphores. Data moves between devices by JAX's collectives and lax.ppermute only.
A program may use at most 128 MiB of HBM per device.

```python
import jax
import jax.numpy as jnp
from jax import lax

C = 64
GW = 8
HALF = 64
ROWS_DEV = 32
NCOL = 1024
TAPS = 129
GROUPS = 8
ROWS = 8192
N_STRIP = 256


def block_scale(key, extent, split, smallest, largest):
    loudness, own = 1.0, jax.random.fold_in(key, 6)
    for position, shards_of in split:
        heights = jnp.exp(jax.random.uniform(jax.random.fold_in(own, position), (shards_of,), jnp.float32, smallest / len(split), largest / len(split)))
        loudness = loudness * jnp.repeat(heights, extent[position] // shards_of).reshape([-1 if axis == position else 1 for axis in range(len(extent))])
    return loudness


def bell_draw(own_key, dims, deviation, most, cuts=(), dtype=jnp.bfloat16):
    loudness = block_scale(own_key, dims, cuts, -0.22, 0.18) if cuts else 1.0
    drawn = jax.random.normal(own_key, dims, jnp.float32) * deviation * loudness
    return jnp.minimum(jnp.maximum(drawn, -most), most).astype(dtype)


def setup_inputs(seed: int = 0) -> dict:
    arg_keys = jax.random.split(jax.random.key(seed), 5)
    return {
        "features": bell_draw(arg_keys[0], (C, ROWS, NCOL), 1.0, 6.0, ((1, 256),)),
        "row_kernel": bell_draw(arg_keys[1], (GROUPS, GW, GW, TAPS), (GW * TAPS) ** -0.5, 0.1875),
        "mix_weight": bell_draw(arg_keys[2], (C, C), C ** -0.5, 0.75),
        "channel_bias": bell_draw(arg_keys[3], (C,), 0.5, 3.0, (), jnp.float32),
    }


def reference(features, row_kernel, mix_weight, channel_bias):
    grid_rows = ROWS_DEV * N_STRIP
    tap_count = 2 * HALF + 1
    front = row_kernel[..., HALF::-1]
    back = row_kernel[..., 2 * HALF:HALF:-1]
    middle = jnp.zeros((GROUPS, GW, GW, grid_rows - tap_count), jnp.bfloat16)
    filters = jnp.concatenate([front, middle, back], axis=-1).astype(jnp.float32)
    spectra = jnp.fft.rfft(filters, axis=-1)
    grouped = features.astype(jnp.float32).reshape(GROUPS, GW, grid_rows, NCOL)

    def one_group(pair):
        block, spectrum = pair
        block_hat = jnp.fft.rfft(block, axis=1)
        out_hat = jnp.einsum("oif,ifw->ofw", spectrum, block_hat)
        return jnp.fft.irfft(out_hat, n=grid_rows, axis=1)

    conv = lax.map(one_group, (grouped, spectra)).reshape(C, grid_rows, NCOL)
    mixed = jnp.einsum("io,irw->orw", mix_weight.astype(jnp.float32), features.astype(jnp.float32))
    total = conv + mixed + channel_bias[:, None, None]
    return jax.nn.gelu(total).astype(jnp.bfloat16)
```

```python
import jax
import jax.numpy as jnp
from jax import lax
from jax.experimental import pallas as pl
from jax.experimental.pallas import tpu as pltpu
from jax.sharding import PartitionSpec as P

FAR, RING_TWIN, OWN, TWIN, RING = range(5)
FAR_CHUNKS = (3, 2, 2, 1)


def banded_kernel(odd_ref, rows_ref, out_ref):
    roles, lanes = out_ref.shape[1:3]
    width = rows_ref.shape[2]
    rows = lanes // width
    shape = (rows, lanes)
    row = lax.broadcasted_iota(jnp.int32, shape, 0)
    column = lax.rem(lax.broadcasted_iota(jnp.int32, shape, 1), rows)
    keep = column >= row
    odd = odd_ref[0]
    for role in range(roles):
        place = jnp.where(odd == 1, roles - 1 - role, role)
        for o in range(width):
            now = jnp.broadcast_to(rows_ref[0, place + 1, o : o + 1, :], shape)
            before = jnp.broadcast_to(rows_ref[0, place, o : o + 1, :], shape)
            now = pltpu.roll(now, 0, 1, stride=1, stride_axis=0)
            before = pltpu.roll(before, lanes - rows, 1, stride=1, stride_axis=0)
            out_ref[0, role, o * rows : (o + 1) * rows, :] = jnp.where(keep, now, before).astype(
                jnp.bfloat16
            )


def banded_matrices(row_kernel, odd, strip_rows):
    groups, width, _, taps = row_kernel.shape
    places = (taps - 1) // strip_rows + 1
    padded = jnp.pad(
        row_kernel.astype(jnp.float32),
        ((0, 0), (0, 0), (0, 0), (strip_rows, places * strip_rows - taps)),
    )
    lanes = width * strip_rows
    rows = padded.reshape(groups, width, width, places + 1, strip_rows)
    rows = jnp.transpose(rows, (0, 3, 1, 2, 4)).reshape(groups, places + 1, width, lanes)
    return pl.pallas_call(
        banded_kernel,
        grid=(groups,),
        in_specs=[
            pl.BlockSpec(memory_space=pltpu.SMEM),
            pl.BlockSpec((1, places + 1, width, lanes), lambda g: (g, 0, 0, 0)),
        ],
        out_specs=pl.BlockSpec((1, places, lanes, lanes), lambda g: (g, 0, 0, 0)),
        out_shape=jax.ShapeDtypeStruct((groups, places, lanes, lanes), jnp.bfloat16),
        cost_estimate=pl.CostEstimate(flops=10**9, bytes_accessed=4 * 10**6, transcendentals=0),
        name="banded",
    )(odd, rows)


def mix_kernel(bias_ref, weight_ref, x_ref, out_ref, wide_ref):
    channels, part, columns = x_ref.shape
    size = channels * part

    @pl.when((pl.program_id(0) == 0) & (pl.program_id(1) == 0))
    def _():
        spread = lax.broadcasted_iota(jnp.int32, (size, channels), 0) // part
        spread = (spread == lax.broadcasted_iota(jnp.int32, (size, channels), 1)).astype(jnp.float32)
        spread = spread.astype(jnp.bfloat16)
        weight = weight_ref[...]
        tall = lax.dot_general(
            spread, weight, (((1,), (1,)), ((), ())), preferred_element_type=jnp.float32
        ).astype(jnp.bfloat16)
        wide = lax.dot_general(
            tall, spread, (((1,), (1,)), ((), ())), preferred_element_type=jnp.float32
        )
        row = lax.broadcasted_iota(jnp.int32, (size, size), 0) % part
        column = lax.broadcasted_iota(jnp.int32, (size, size), 1) % part
        wide_ref[...] = jnp.where(row == column, wide, 0.0).astype(jnp.bfloat16)

    x = x_ref[...].astype(jnp.float32).reshape(size, columns).astype(jnp.bfloat16)
    total = jnp.dot(wide_ref[...], x, preferred_element_type=jnp.float32)
    for c in range(channels):
        out_ref[c] = total[c * part : (c + 1) * part] + bias_ref[c]


def mix(features, mix_weight, channel_bias):
    channels, rows, columns = features.shape
    part = 8
    half = columns // 2
    block = pl.BlockSpec((channels, part, half), lambda t, h: (0, t, h))
    return pl.pallas_call(
        mix_kernel,
        grid=(rows // part, 2),
        in_specs=[
            pl.BlockSpec(memory_space=pltpu.SMEM),
            pl.BlockSpec((channels, channels), lambda t, h: (0, 0)),
            block,
        ],
        out_specs=block,
        out_shape=jax.ShapeDtypeStruct(features.shape, jnp.float32),
        scratch_shapes=[pltpu.VMEM((channels * part, channels * part), jnp.bfloat16)],
        cost_estimate=pl.CostEstimate(
            flops=2 * part * channels * features.size,
            bytes_accessed=6 * features.size,
            transcendentals=0,
        ),
        name="mix",
    )(channel_bias, mix_weight, features)


def pair_kernel(first_matrix_ref, second_matrix_ref, first_ref, second_ref, part_ref, out_ref):
    width, rows, columns = first_ref.shape
    flat = (width * rows, columns)
    total = jnp.dot(
        first_matrix_ref[0, 0], first_ref[...].reshape(flat), preferred_element_type=jnp.float32
    )
    total += jnp.dot(
        second_matrix_ref[0, 0], second_ref[...].reshape(flat), preferred_element_type=jnp.float32
    )
    out_ref[...] = part_ref[...] + total.reshape(width, rows, columns)


def add_pair(matrices, first, first_role, second, second_role, part):
    groups, _, lanes, _ = matrices.shape
    channels, rows, columns = first.shape
    width = channels // groups
    strip = pl.BlockSpec((width, rows, columns), lambda g: (g, 0, 0))
    return pl.pallas_call(
        pair_kernel,
        grid=(groups,),
        in_specs=[
            pl.BlockSpec((1, 1, lanes, lanes), lambda g: (g, first_role, 0, 0)),
            pl.BlockSpec((1, 1, lanes, lanes), lambda g: (g, second_role, 0, 0)),
            strip,
            strip,
            strip,
        ],
        out_specs=strip,
        out_shape=jax.ShapeDtypeStruct(part.shape, jnp.float32),
        input_output_aliases={4: 0},
        cost_estimate=pl.CostEstimate(
            flops=4 * lanes * first.size, bytes_accessed=12 * first.size, transcendentals=0
        ),
    )(matrices, matrices, first, second, part)


def last_kernel(matrix_ref, far_ref, part_ref, *refs):
    out_ref = refs[-1]
    width, rows, columns = far_ref.shape
    total = jnp.dot(
        matrix_ref[0, 0],
        far_ref[...].reshape(width * rows, columns),
        preferred_element_type=jnp.float32,
    )
    total = part_ref[...] + total.reshape(width, rows, columns)
    out_ref[...] = jax.nn.gelu(total).astype(jnp.bfloat16)


def finish(matrices, far, part, out, start, count):
    groups, _, lanes, _ = matrices.shape
    channels, rows, columns = part.shape
    width = channels // groups
    here = pl.BlockSpec((width, rows, columns), lambda g: (g + start, 0, 0))
    given = [] if out is None else [out]
    return pl.pallas_call(
        last_kernel,
        grid=(count,),
        in_specs=[
            pl.BlockSpec((1, 1, lanes, lanes), lambda g: (g + start, FAR, 0, 0)),
            pl.BlockSpec((width, rows, columns), lambda g: (g, 0, 0)),
            here,
        ]
        + [pl.BlockSpec(memory_space=pl.ANY)] * len(given),
        out_specs=here,
        out_shape=jax.ShapeDtypeStruct(part.shape, jnp.bfloat16),
        input_output_aliases={3: 0} if given else {},
        cost_estimate=pl.CostEstimate(
            flops=2 * lanes * far.size, bytes_accessed=8 * far.size, transcendentals=far.size
        ),
    )(matrices, far, part, *given)


def local(features, row_kernel, mix_weight, channel_bias):
    _, strip_rows, _ = features.shape
    _, width = row_kernel.shape[:2]
    devices = lax.axis_size("strip")
    odd = lax.rem(lax.axis_index("strip"), 2).reshape(1)
    ring_route = [(i, (i + (2 if i % 2 else -2)) % devices) for i in range(devices)]
    far_route = [(i, (i + (1 if i % 2 else -1)) % devices) for i in range(devices)]
    twin_route = [(i, i ^ 1) for i in range(devices)]
    ring = lax.ppermute(features, "strip", ring_route)
    twin = lax.ppermute(features, "strip", twin_route)
    fars = []
    start = 0
    for count in FAR_CHUNKS:
        piece = twin[start * width : (start + count) * width]
        fars.append(lax.ppermute(piece, "strip", far_route))
        start += count
    ring_twin = lax.ppermute(ring, "strip", twin_route)
    matrices = banded_matrices(row_kernel, odd, strip_rows)
    part = mix(features, mix_weight, channel_bias)
    part = add_pair(matrices, features, OWN, twin, TWIN, part)
    part = add_pair(matrices, ring, RING, ring_twin, RING_TWIN, part)
    out = None
    start = 0
    for far, count in zip(fars, FAR_CHUNKS):
        out = finish(matrices, far, part, out, start, count)
        start += count
    return out


def solution(mesh):
    return jax.shard_map(
        local,
        mesh=mesh,
        in_specs=(P(None, "strip", None), P(), P(), P()),
        out_specs=P(None, "strip", None),
        check_vma=False,
    )
```

```python
import functools

import jax
import jax.numpy as jnp
from jax import lax
from jax.experimental import pallas as pl
from jax.experimental.pallas import tpu as pltpu
from jax.sharding import PartitionSpec as P

FAR, RING_TWIN, OWN, TWIN, RING = range(5)
FAR_CHUNKS = (4, 3, 1)
WHOLE = pl.BlockSpec(memory_space=pltpu.VMEM)
GRANT = pltpu.CompilerParams(vmem_limit_bytes=16 * 2**20)


def banded_kernel(odd_ref, rows_ref, out_ref):
    g = pl.program_id(0)
    roles, lanes = out_ref.shape[1:3]
    width = rows_ref.shape[2]
    rows = lanes // width
    shape = (rows, lanes)
    row = lax.broadcasted_iota(jnp.int32, shape, 0)
    column = lax.rem(lax.broadcasted_iota(jnp.int32, shape, 1), rows)
    keep = column >= row
    odd = odd_ref[0]
    for role in range(roles):
        place = jnp.where(odd == 1, roles - 1 - role, role)
        for o in range(width):
            now = jnp.broadcast_to(rows_ref[0, place + 1, o : o + 1, :], shape)
            before = jnp.broadcast_to(rows_ref[0, place, o : o + 1, :], shape)
            now = pltpu.roll(now, 0, 1, stride=1, stride_axis=0)
            before = pltpu.roll(before, lanes - rows, 1, stride=1, stride_axis=0)
            out_ref[g, role, o * rows : (o + 1) * rows, :] = jnp.where(keep, now, before).astype(
                jnp.bfloat16
            )


def banded_matrices(row_kernel, odd, strip_rows):
    groups, width, _, taps = row_kernel.shape
    places = (taps - 1) // strip_rows + 1
    padded = jnp.pad(
        row_kernel.astype(jnp.float32),
        ((0, 0), (0, 0), (0, 0), (strip_rows, places * strip_rows - taps)),
    )
    lanes = width * strip_rows
    rows = padded.reshape(groups, width, width, places + 1, strip_rows)
    rows = jnp.transpose(rows, (0, 3, 1, 2, 4)).reshape(groups, places + 1, width, lanes)
    return pl.pallas_call(
        banded_kernel,
        grid=(groups,),
        in_specs=[
            pl.BlockSpec(memory_space=pltpu.SMEM),
            pl.BlockSpec((1, places + 1, width, lanes), lambda g: (g, 0, 0, 0)),
        ],
        out_specs=WHOLE,
        out_shape=pltpu.VMEM((groups, places, lanes, lanes), jnp.bfloat16),
        compiler_params=GRANT,
        cost_estimate=pl.CostEstimate(flops=10**9, bytes_accessed=4 * 10**6, transcendentals=0),
        name="banded",
    )(odd, rows)


def mix_kernel(bias_ref, weight_ref, x_ref, out_ref, wide_ref):
    channels, part, columns = x_ref.shape
    size = channels * part

    @pl.when((pl.program_id(0) == 0) & (pl.program_id(1) == 0))
    def _():
        spread = lax.broadcasted_iota(jnp.int32, (size, channels), 0) // part
        spread = (spread == lax.broadcasted_iota(jnp.int32, (size, channels), 1)).astype(jnp.float32)
        spread = spread.astype(jnp.bfloat16)
        weight = weight_ref[...]
        tall = lax.dot_general(
            spread, weight, (((1,), (1,)), ((), ())), preferred_element_type=jnp.float32
        ).astype(jnp.bfloat16)
        wide = lax.dot_general(
            tall, spread, (((1,), (1,)), ((), ())), preferred_element_type=jnp.float32
        )
        row = lax.broadcasted_iota(jnp.int32, (size, size), 0) % part
        column = lax.broadcasted_iota(jnp.int32, (size, size), 1) % part
        wide_ref[...] = jnp.where(row == column, wide, 0.0).astype(jnp.bfloat16)

    x = x_ref[...].astype(jnp.float32).reshape(size, columns).astype(jnp.bfloat16)
    total = jnp.dot(wide_ref[...], x, preferred_element_type=jnp.float32)
    rows = pl.ds(pl.multiple_of(pl.program_id(0) * part, part), part)
    lanes = pl.ds(pl.multiple_of(pl.program_id(1) * columns, columns), columns)
    for c in range(channels):
        out_ref[c, rows, lanes] = total[c * part : (c + 1) * part] + bias_ref[c]


def mix(features, mix_weight, channel_bias):
    channels, rows, columns = features.shape
    part = 8
    half = columns // 2
    block = pl.BlockSpec((channels, part, half), lambda t, h: (0, t, h))
    return pl.pallas_call(
        mix_kernel,
        grid=(rows // part, 2),
        in_specs=[
            pl.BlockSpec(memory_space=pltpu.SMEM),
            pl.BlockSpec((channels, channels), lambda t, h: (0, 0)),
            block,
        ],
        out_specs=WHOLE,
        out_shape=pltpu.VMEM(features.shape, jnp.float32),
        compiler_params=GRANT,
        scratch_shapes=[pltpu.VMEM((channels * part, channels * part), jnp.bfloat16)],
        cost_estimate=pl.CostEstimate(
            flops=2 * part * channels * features.size,
            bytes_accessed=6 * features.size,
            transcendentals=0,
        ),
        name="mix",
    )(channel_bias, mix_weight, features)


def pair_kernel(first_role, second_role, matrix_ref, first_ref, second_ref, part_ref, out_ref):
    g = pl.program_id(0)
    width, rows, columns = first_ref.shape
    flat = (width * rows, columns)
    total = jnp.dot(
        matrix_ref[g, first_role], first_ref[...].reshape(flat), preferred_element_type=jnp.float32
    )
    total += jnp.dot(
        matrix_ref[g, second_role], second_ref[...].reshape(flat), preferred_element_type=jnp.float32
    )
    here = pl.ds(g * width, width)
    out_ref[here] = part_ref[here] + total.reshape(width, rows, columns)


def add_pair(matrices, first, first_role, second, second_role, part):
    groups, _, lanes, _ = matrices.shape
    channels, rows, columns = first.shape
    width = channels // groups
    strip = pl.BlockSpec((width, rows, columns), lambda g: (g, 0, 0))
    return pl.pallas_call(
        functools.partial(pair_kernel, first_role, second_role),
        grid=(groups,),
        in_specs=[WHOLE, strip, strip, WHOLE],
        out_specs=WHOLE,
        out_shape=pltpu.VMEM(part.shape, jnp.float32),
        input_output_aliases={3: 0},
        compiler_params=GRANT,
        cost_estimate=pl.CostEstimate(
            flops=4 * lanes * first.size, bytes_accessed=4 * first.size, transcendentals=0
        ),
    )(matrices, first, second, part)


def last_kernel(start, count, matrix_ref, part_ref, far_ref, *refs):
    out_ref, ready_ref, sems = refs[-3:]
    width = ready_ref.shape[0] // count
    rows, columns = ready_ref.shape[1:]
    tile = columns // 2

    def copy(g, t):
        lanes = pl.ds(t * tile, tile)
        return pltpu.make_async_copy(
            ready_ref.at[pl.ds(g * width, width), :, lanes],
            out_ref.at[pl.ds((start + g) * width, width), :, lanes],
            sems.at[2 * g + t],
        )

    def group(g):
        here = pl.ds(g * width, width)
        for t in range(2):
            lanes = slice(t * tile, (t + 1) * tile)
            total = jnp.dot(
                matrix_ref[start + g, FAR],
                far_ref[here, :, lanes].reshape(width * rows, tile),
                preferred_element_type=jnp.float32,
            )
            total = part_ref[pl.ds((start + g) * width, width), :, lanes] + total.reshape(
                width, rows, tile
            )
            ready_ref[here, :, lanes] = jax.nn.gelu(total).astype(jnp.bfloat16)
            copy(g, t).start()

    if count == 1:
        group(0)
    else:
        pl.loop(0, count)(group)
    for g in range(count):
        for t in range(2):
            copy(g, t).wait()


def finish(matrices, part, far, out, start, count):
    groups, _, lanes, _ = matrices.shape
    channels, rows, columns = part.shape
    width = channels // groups
    given = [] if out is None else [out]
    whole = pl.BlockSpec(memory_space=pl.ANY)
    return pl.pallas_call(
        functools.partial(last_kernel, start, count),
        in_specs=[WHOLE] * 3 + [whole] * len(given),
        out_specs=whole,
        out_shape=jax.ShapeDtypeStruct(part.shape, jnp.bfloat16),
        input_output_aliases={3: 0} if given else {},
        scratch_shapes=[
            pltpu.VMEM((count * width, rows, columns), jnp.bfloat16),
            pltpu.SemaphoreType.DMA((2 * count,)),
        ],
        compiler_params=GRANT,
        cost_estimate=pl.CostEstimate(
            flops=2 * lanes * far.size, bytes_accessed=4 * far.size, transcendentals=far.size
        ),
    )(matrices, part, far, *given)


def local(features, row_kernel, mix_weight, channel_bias):
    strip_rows = features.shape[1]
    width = row_kernel.shape[1]
    devices = lax.axis_size("strip")
    odd = lax.rem(lax.axis_index("strip"), 2).reshape(1)
    ring_route = [(i, (i + (2 if i % 2 else -2)) % devices) for i in range(devices)]
    far_route = [(i, (i + (1 if i % 2 else -1)) % devices) for i in range(devices)]
    twin_route = [(i, i ^ 1) for i in range(devices)]
    ring = lax.ppermute(features, "strip", ring_route)
    twin = lax.ppermute(features, "strip", twin_route)
    fars = []
    start = 0
    for count in FAR_CHUNKS:
        piece = twin[start * width : (start + count) * width]
        fars.append(lax.ppermute(piece, "strip", far_route))
        start += count
    ring_twin = lax.ppermute(ring, "strip", twin_route)
    matrices = banded_matrices(row_kernel, odd, strip_rows)
    part = mix(features, mix_weight, channel_bias)
    part = add_pair(matrices, features, OWN, twin, TWIN, part)
    part = add_pair(matrices, ring, RING, ring_twin, RING_TWIN, part)
    out = None
    start = 0
    for far, count in zip(fars, FAR_CHUNKS):
        out = finish(matrices, part, far, out, start, count)
        start += count
    return out


def solution(mesh):
    return jax.shard_map(
        local,
        mesh=mesh,
        in_specs=(P(None, "strip", None), P(), P(), P()),
        out_specs=P(None, "strip", None),
        check_vma=False,
    )
```

```python
import functools

import jax
import jax.numpy as jnp
from jax import lax
from jax.experimental import pallas as pl
from jax.experimental.pallas import tpu as pltpu
from jax.sharding import PartitionSpec as P

FAR, RING_TWIN, OWN, TWIN, RING = range(5)
FAR_CHUNKS = (4, 3)
WHOLE = pl.BlockSpec(memory_space=pltpu.VMEM)
GRANT = pltpu.CompilerParams(vmem_limit_bytes=16 * 2**20)


def banded_kernel(odd_ref, rows_ref, out_ref):
    g = pl.program_id(0)
    roles, lanes = out_ref.shape[1:3]
    width = rows_ref.shape[2]
    rows = lanes // width
    shape = (rows, lanes)
    row = lax.broadcasted_iota(jnp.int32, shape, 0)
    column = lax.rem(lax.broadcasted_iota(jnp.int32, shape, 1), rows)
    keep = column >= row
    odd = odd_ref[0]
    for role in range(roles):
        place = jnp.where(odd == 1, roles - 1 - role, role)
        for o in range(width):
            now = jnp.broadcast_to(rows_ref[0, place + 1, o : o + 1, :], shape)
            before = jnp.broadcast_to(rows_ref[0, place, o : o + 1, :], shape)
            now = pltpu.roll(now, 0, 1, stride=1, stride_axis=0)
            before = pltpu.roll(before, lanes - rows, 1, stride=1, stride_axis=0)
            out_ref[g, role, o * rows : (o + 1) * rows, :] = jnp.where(keep, now, before).astype(
                jnp.bfloat16
            )


def banded_matrices(row_kernel, odd, strip_rows):
    groups, width, _, taps = row_kernel.shape
    places = (taps - 1) // strip_rows + 1
    padded = jnp.pad(
        row_kernel.astype(jnp.float32),
        ((0, 0), (0, 0), (0, 0), (strip_rows, places * strip_rows - taps)),
    )
    lanes = width * strip_rows
    rows = padded.reshape(groups, width, width, places + 1, strip_rows)
    rows = jnp.transpose(rows, (0, 3, 1, 2, 4)).reshape(groups, places + 1, width, lanes)
    return pl.pallas_call(
        banded_kernel,
        grid=(groups,),
        in_specs=[
            pl.BlockSpec(memory_space=pltpu.SMEM),
            pl.BlockSpec((1, places + 1, width, lanes), lambda g: (g, 0, 0, 0)),
        ],
        out_specs=WHOLE,
        out_shape=pltpu.VMEM((groups, places, lanes, lanes), jnp.bfloat16),
        compiler_params=GRANT,
        cost_estimate=pl.CostEstimate(flops=10**9, bytes_accessed=4 * 10**6, transcendentals=0),
        name="banded",
    )(odd, rows)


def mix_kernel(bias_ref, weight_ref, x_ref, out_ref, wide_ref):
    channels, part, columns = x_ref.shape
    size = channels * part

    @pl.when((pl.program_id(0) == 0) & (pl.program_id(1) == 0))
    def _():
        spread = lax.broadcasted_iota(jnp.int32, (size, channels), 0) // part
        spread = (spread == lax.broadcasted_iota(jnp.int32, (size, channels), 1)).astype(jnp.float32)
        spread = spread.astype(jnp.bfloat16)
        weight = weight_ref[...]
        tall = lax.dot_general(
            spread, weight, (((1,), (1,)), ((), ())), preferred_element_type=jnp.float32
        ).astype(jnp.bfloat16)
        wide = lax.dot_general(
            tall, spread, (((1,), (1,)), ((), ())), preferred_element_type=jnp.float32
        )
        row = lax.broadcasted_iota(jnp.int32, (size, size), 0) % part
        column = lax.broadcasted_iota(jnp.int32, (size, size), 1) % part
        wide_ref[...] = jnp.where(row == column, wide, 0.0).astype(jnp.bfloat16)

    x = x_ref[...].astype(jnp.float32).reshape(size, columns).astype(jnp.bfloat16)
    total = jnp.dot(wide_ref[...], x, preferred_element_type=jnp.float32)
    rows = pl.ds(pl.multiple_of(pl.program_id(0) * part, part), part)
    lanes = pl.ds(pl.multiple_of(pl.program_id(1) * columns, columns), columns)
    for c in range(channels):
        out_ref[c, rows, lanes] = total[c * part : (c + 1) * part] + bias_ref[c]


def mix(features, mix_weight, channel_bias):
    channels, rows, columns = features.shape
    part = 8
    half = columns // 2
    block = pl.BlockSpec((channels, part, half), lambda t, h: (0, t, h))
    return pl.pallas_call(
        mix_kernel,
        grid=(rows // part, 2),
        in_specs=[
            pl.BlockSpec(memory_space=pltpu.SMEM),
            pl.BlockSpec((channels, channels), lambda t, h: (0, 0)),
            block,
        ],
        out_specs=WHOLE,
        out_shape=pltpu.VMEM(features.shape, jnp.float32),
        compiler_params=GRANT,
        scratch_shapes=[pltpu.VMEM((channels * part, channels * part), jnp.bfloat16)],
        cost_estimate=pl.CostEstimate(
            flops=2 * part * channels * features.size,
            bytes_accessed=6 * features.size,
            transcendentals=0,
        ),
        name="mix",
    )(channel_bias, mix_weight, features)


def pair_kernel(first_role, second_role, matrix_ref, first_ref, second_ref, part_ref, out_ref):
    g = pl.program_id(0)
    width, rows, columns = first_ref.shape
    flat = (width * rows, columns)
    total = jnp.dot(
        matrix_ref[g, first_role], first_ref[...].reshape(flat), preferred_element_type=jnp.float32
    )
    total += jnp.dot(
        matrix_ref[g, second_role], second_ref[...].reshape(flat), preferred_element_type=jnp.float32
    )
    here = pl.ds(g * width, width)
    out_ref[here] = part_ref[here] + total.reshape(width, rows, columns)


def add_pair(matrices, first, first_role, second, second_role, part):
    groups, _, lanes, _ = matrices.shape
    channels, rows, columns = first.shape
    width = channels // groups
    strip = pl.BlockSpec((width, rows, columns), lambda g: (g, 0, 0))
    return pl.pallas_call(
        functools.partial(pair_kernel, first_role, second_role),
        grid=(groups,),
        in_specs=[WHOLE, strip, strip, WHOLE],
        out_specs=WHOLE,
        out_shape=pltpu.VMEM(part.shape, jnp.float32),
        input_output_aliases={3: 0},
        compiler_params=GRANT,
        cost_estimate=pl.CostEstimate(
            flops=4 * lanes * first.size, bytes_accessed=4 * first.size, transcendentals=0
        ),
    )(matrices, first, second, part)


def last_kernel(start, count, cuts, matrix_ref, part_ref, *refs):
    out_ref, ready_ref, sems = refs[-3:]
    width = ready_ref.shape[0] // count
    rows, columns = ready_ref.shape[1:]
    edges = [0, columns // 2, columns] if cuts is None else cuts
    tiles = list(zip(edges, edges[1:]))

    def far(g, t):
        lanes = slice(*tiles[t])
        if cuts is None:
            return refs[0][pl.ds(g * width, width), :, lanes]
        if t == 0:
            return refs[0][...]
        return refs[2 * t - 1][...] + refs[2 * t][...]

    def copy(g, t):
        lanes = pl.ds(tiles[t][0], tiles[t][1] - tiles[t][0])
        return pltpu.make_async_copy(
            ready_ref.at[pl.ds(g * width, width), :, lanes],
            out_ref.at[pl.ds((start + g) * width, width), :, lanes],
            sems.at[len(tiles) * g + t],
        )

    def group(g):
        for t, (first, last) in enumerate(tiles):
            lanes = slice(first, last)
            total = jnp.dot(
                matrix_ref[start + g, FAR],
                far(g, t).reshape(width * rows, last - first),
                preferred_element_type=jnp.float32,
            )
            total = part_ref[pl.ds((start + g) * width, width), :, lanes] + total.reshape(
                width, rows, last - first
            )
            ready_ref[pl.ds(g * width, width), :, lanes] = jax.nn.gelu(total).astype(jnp.bfloat16)
            copy(g, t).start()

    if count == 1:
        group(0)
    else:
        pl.loop(0, count)(group)
    for g in range(count):
        for t in range(len(tiles)):
            copy(g, t).wait()


def finish(matrices, part, fars, out, start, count, cuts):
    groups, _, lanes, _ = matrices.shape
    channels, rows, columns = part.shape
    width = channels // groups
    given = [] if out is None else [out]
    whole = pl.BlockSpec(memory_space=pl.ANY)
    size = count * width * rows * columns
    return pl.pallas_call(
        functools.partial(last_kernel, start, count, cuts),
        in_specs=[WHOLE] * (2 + len(fars)) + [whole] * len(given),
        out_specs=whole,
        out_shape=jax.ShapeDtypeStruct(part.shape, jnp.bfloat16),
        input_output_aliases={2 + len(fars): 0} if given else {},
        scratch_shapes=[
            pltpu.VMEM((count * width, rows, columns), jnp.bfloat16),
            pltpu.SemaphoreType.DMA((3 * count,)),
        ],
        compiler_params=GRANT,
        cost_estimate=pl.CostEstimate(
            flops=2 * lanes * size, bytes_accessed=4 * size, transcendentals=size
        ),
    )(matrices, part, *fars, *given)


def relay_hops(devices):
    if devices != 256:
        return [], [], []

    def strip(x, z, y, core):
        return ((x % 4 * 8 + z % 8) * 4 + y) * 2 + core

    paths = []
    for x in range(4):
        low, high = strip(x - 1, 7, 3, 1), strip(x, 0, 0, 0)
        paths.append([low, strip(x - 1, 6, 3, 1), strip(x, 6, 0, 1), high])
        paths.append([high, strip(x, 1, 0, 1), strip(x - 1, 1, 3, 1), low])
    return tuple([tuple(path[i : i + 2]) for path in paths] for i in range(3))


def local(features, row_kernel, mix_weight, channel_bias):
    strip_rows, columns = features.shape[1:]
    width = row_kernel.shape[1]
    devices = lax.axis_size("strip")
    odd = lax.rem(lax.axis_index("strip"), 2).reshape(1)
    ring_route = [(i, (i + (2 if i % 2 else -2)) % devices) for i in range(devices)]
    far_route = [(i, (i + (1 if i % 2 else -1)) % devices) for i in range(devices)]
    twin_route = [(i, i ^ 1) for i in range(devices)]
    ring = lax.ppermute(features, "strip", ring_route)
    twin = lax.ppermute(features, "strip", twin_route)
    fars = []
    start = 0
    for count in FAR_CHUNKS:
        piece = twin[start * width : (start + count) * width]
        fars.append(lax.ppermute(piece, "strip", far_route))
        start += count
    end = twin[start * width :]
    cuts = [0, 5 * columns // 8, columns]
    ends = [lax.ppermute(end[:, :, : cuts[1]], "strip", far_route)]
    piece = end[:, :, cuts[1] :]
    hops = relay_hops(devices)
    relayed = [target for _, target in hops[2]]
    route = [pair for pair in far_route if pair[1] not in relayed]
    ends.append(lax.ppermute(piece, "strip", route))
    for hop in hops:
        piece = lax.ppermute(piece, "strip", hop)
    ends.append(piece)
    ring_twin = lax.ppermute(ring, "strip", twin_route)
    matrices = banded_matrices(row_kernel, odd, strip_rows)
    part = mix(features, mix_weight, channel_bias)
    part = add_pair(matrices, features, OWN, twin, TWIN, part)
    part = add_pair(matrices, ring, RING, ring_twin, RING_TWIN, part)
    out = None
    start = 0
    for far, count in zip(fars, FAR_CHUNKS):
        out = finish(matrices, part, [far], out, start, count, None)
        start += count
    return finish(matrices, part, ends, out, start, 1, cuts)


def solution(mesh):
    return jax.shard_map(
        local,
        mesh=mesh,
        in_specs=(P(None, "strip", None), P(), P(), P()),
        out_specs=P(None, "strip", None),
        check_vma=False,
    )
```

```python
import functools

import jax
import jax.numpy as jnp
from jax import lax
from jax.experimental import pallas as pl
from jax.experimental.pallas import tpu as pltpu
from jax.sharding import PartitionSpec as P

FAR, RING_TWIN, OWN, TWIN, RING = range(5)
FAR_CHUNKS = (4, 3)
RELAY_PLANES = ((5, 1), (6, 2))
WHOLE = pl.BlockSpec(memory_space=pltpu.VMEM)
GRANT = pltpu.CompilerParams(vmem_limit_bytes=16 * 2**20)


def banded_kernel(odd_ref, rows_ref, out_ref):
    g = pl.program_id(0)
    roles, lanes = out_ref.shape[1:3]
    width = rows_ref.shape[2]
    rows = lanes // width
    shape = (rows, lanes)
    row = lax.broadcasted_iota(jnp.int32, shape, 0)
    column = lax.rem(lax.broadcasted_iota(jnp.int32, shape, 1), rows)
    keep = column >= row
    odd = odd_ref[0]
    for role in range(roles):
        place = jnp.where(odd == 1, roles - 1 - role, role)
        for o in range(width):
            now = jnp.broadcast_to(rows_ref[0, place + 1, o : o + 1, :], shape)
            before = jnp.broadcast_to(rows_ref[0, place, o : o + 1, :], shape)
            now = pltpu.roll(now, 0, 1, stride=1, stride_axis=0)
            before = pltpu.roll(before, lanes - rows, 1, stride=1, stride_axis=0)
            out_ref[g, role, o * rows : (o + 1) * rows, :] = jnp.where(keep, now, before).astype(
                jnp.bfloat16
            )


def banded_matrices(row_kernel, odd, strip_rows):
    groups, width, _, taps = row_kernel.shape
    places = (taps - 1) // strip_rows + 1
    padded = jnp.pad(
        row_kernel.astype(jnp.float32),
        ((0, 0), (0, 0), (0, 0), (strip_rows, places * strip_rows - taps)),
    )
    lanes = width * strip_rows
    rows = padded.reshape(groups, width, width, places + 1, strip_rows)
    rows = jnp.transpose(rows, (0, 3, 1, 2, 4)).reshape(groups, places + 1, width, lanes)
    return pl.pallas_call(
        banded_kernel,
        grid=(groups,),
        in_specs=[
            pl.BlockSpec(memory_space=pltpu.SMEM),
            pl.BlockSpec((1, places + 1, width, lanes), lambda g: (g, 0, 0, 0)),
        ],
        out_specs=WHOLE,
        out_shape=pltpu.VMEM((groups, places, lanes, lanes), jnp.bfloat16),
        compiler_params=GRANT,
        cost_estimate=pl.CostEstimate(flops=10**9, bytes_accessed=4 * 10**6, transcendentals=0),
        name="banded",
    )(odd, rows)


def mix_kernel(bias_ref, weight_ref, x_ref, out_ref, wide_ref):
    channels, part, columns = x_ref.shape
    size = channels * part

    @pl.when((pl.program_id(0) == 0) & (pl.program_id(1) == 0))
    def _():
        spread = lax.broadcasted_iota(jnp.int32, (size, channels), 0) // part
        spread = (spread == lax.broadcasted_iota(jnp.int32, (size, channels), 1)).astype(jnp.float32)
        spread = spread.astype(jnp.bfloat16)
        weight = weight_ref[...]
        tall = lax.dot_general(
            spread, weight, (((1,), (1,)), ((), ())), preferred_element_type=jnp.float32
        ).astype(jnp.bfloat16)
        wide = lax.dot_general(
            tall, spread, (((1,), (1,)), ((), ())), preferred_element_type=jnp.float32
        )
        row = lax.broadcasted_iota(jnp.int32, (size, size), 0) % part
        column = lax.broadcasted_iota(jnp.int32, (size, size), 1) % part
        wide_ref[...] = jnp.where(row == column, wide, 0.0).astype(jnp.bfloat16)

    x = x_ref[...].astype(jnp.float32).reshape(size, columns).astype(jnp.bfloat16)
    total = jnp.dot(wide_ref[...], x, preferred_element_type=jnp.float32)
    rows = pl.ds(pl.multiple_of(pl.program_id(0) * part, part), part)
    lanes = pl.ds(pl.multiple_of(pl.program_id(1) * columns, columns), columns)
    for c in range(channels):
        out_ref[c, rows, lanes] = total[c * part : (c + 1) * part] + bias_ref[c]


def mix(features, mix_weight, channel_bias):
    channels, rows, columns = features.shape
    part = 8
    half = columns // 2
    block = pl.BlockSpec((channels, part, half), lambda t, h: (0, t, h))
    return pl.pallas_call(
        mix_kernel,
        grid=(rows // part, 2),
        in_specs=[
            pl.BlockSpec(memory_space=pltpu.SMEM),
            pl.BlockSpec((channels, channels), lambda t, h: (0, 0)),
            block,
        ],
        out_specs=WHOLE,
        out_shape=pltpu.VMEM(features.shape, jnp.float32),
        compiler_params=GRANT,
        scratch_shapes=[pltpu.VMEM((channels * part, channels * part), jnp.bfloat16)],
        cost_estimate=pl.CostEstimate(
            flops=2 * part * channels * features.size,
            bytes_accessed=6 * features.size,
            transcendentals=0,
        ),
        name="mix",
    )(channel_bias, mix_weight, features)


def pair_kernel(first_role, second_role, matrix_ref, first_ref, second_ref, part_ref, out_ref):
    g = pl.program_id(0)
    width, rows, columns = first_ref.shape
    flat = (width * rows, columns)
    total = jnp.dot(
        matrix_ref[g, first_role], first_ref[...].reshape(flat), preferred_element_type=jnp.float32
    )
    total += jnp.dot(
        matrix_ref[g, second_role], second_ref[...].reshape(flat), preferred_element_type=jnp.float32
    )
    here = pl.ds(g * width, width)
    out_ref[here] = part_ref[here] + total.reshape(width, rows, columns)


def add_pair(matrices, first, first_role, second, second_role, part):
    groups, _, lanes, _ = matrices.shape
    channels, rows, columns = first.shape
    width = channels // groups
    strip = pl.BlockSpec((width, rows, columns), lambda g: (g, 0, 0))
    return pl.pallas_call(
        functools.partial(pair_kernel, first_role, second_role),
        grid=(groups,),
        in_specs=[WHOLE, strip, strip, WHOLE],
        out_specs=WHOLE,
        out_shape=pltpu.VMEM(part.shape, jnp.float32),
        input_output_aliases={3: 0},
        compiler_params=GRANT,
        cost_estimate=pl.CostEstimate(
            flops=4 * lanes * first.size, bytes_accessed=4 * first.size, transcendentals=0
        ),
    )(matrices, first, second, part)


def last_kernel(start, count, cuts, matrix_ref, part_ref, *refs):
    out_ref, ready_ref, sems = refs[-3:]
    width = ready_ref.shape[0] // count
    rows, columns = ready_ref.shape[1:]
    edges = [0, columns // 2, columns] if cuts is None else cuts
    tiles = list(zip(edges, edges[1:]))

    def far(g, t):
        lanes = slice(*tiles[t])
        if cuts is None:
            return refs[0][pl.ds(g * width, width), :, lanes]
        if t == 0:
            return refs[0][...]
        return refs[2 * t - 1][...] + refs[2 * t][...]

    def copy(g, t):
        lanes = pl.ds(tiles[t][0], tiles[t][1] - tiles[t][0])
        return pltpu.make_async_copy(
            ready_ref.at[pl.ds(g * width, width), :, lanes],
            out_ref.at[pl.ds((start + g) * width, width), :, lanes],
            sems.at[len(tiles) * g + t],
        )

    def group(g):
        for t, (first, last) in enumerate(tiles):
            lanes = slice(first, last)
            total = jnp.dot(
                matrix_ref[start + g, FAR],
                far(g, t).reshape(width * rows, last - first),
                preferred_element_type=jnp.float32,
            )
            total = part_ref[pl.ds((start + g) * width, width), :, lanes] + total.reshape(
                width, rows, last - first
            )
            ready_ref[pl.ds(g * width, width), :, lanes] = jax.nn.gelu(total).astype(jnp.bfloat16)
            copy(g, t).start()

    if count == 1:
        group(0)
    else:
        pl.loop(0, count)(group)
    for g in range(count):
        for t in range(len(tiles)):
            copy(g, t).wait()


def finish(matrices, part, fars, out, start, count, cuts):
    groups, _, lanes, _ = matrices.shape
    channels, rows, columns = part.shape
    width = channels // groups
    given = [] if out is None else [out]
    whole = pl.BlockSpec(memory_space=pl.ANY)
    size = count * width * rows * columns
    return pl.pallas_call(
        functools.partial(last_kernel, start, count, cuts),
        in_specs=[WHOLE] * (2 + len(fars)) + [whole] * len(given),
        out_specs=whole,
        out_shape=jax.ShapeDtypeStruct(part.shape, jnp.bfloat16),
        input_output_aliases={2 + len(fars): 0} if given else {},
        scratch_shapes=[
            pltpu.VMEM((count * width, rows, columns), jnp.bfloat16),
            pltpu.SemaphoreType.DMA((3 * count,)),
        ],
        compiler_params=GRANT,
        cost_estimate=pl.CostEstimate(
            flops=2 * lanes * size, bytes_accessed=4 * size, transcendentals=size
        ),
    )(matrices, part, *fars, *given)


def relay_hops(devices, up_plane, down_plane):
    if devices != 256:
        return [], [], []

    def strip(x, z, y, core):
        return ((x % 4 * 8 + z % 8) * 4 + y) * 2 + core

    paths = []
    for x in range(4):
        low, high = strip(x - 1, 7, 3, 1), strip(x, 0, 0, 0)
        paths.append([low, strip(x - 1, up_plane, 3, 1), strip(x, up_plane, 0, 1), high])
        paths.append([high, strip(x, down_plane, 0, 1), strip(x - 1, down_plane, 3, 1), low])
    return tuple([tuple(path[i : i + 2]) for path in paths] for i in range(3))


def local(features, row_kernel, mix_weight, channel_bias):
    strip_rows, columns = features.shape[1:]
    width = row_kernel.shape[1]
    devices = lax.axis_size("strip")
    odd = lax.rem(lax.axis_index("strip"), 2).reshape(1)
    ring_route = [(i, (i + (2 if i % 2 else -2)) % devices) for i in range(devices)]
    far_route = [(i, (i + (1 if i % 2 else -1)) % devices) for i in range(devices)]
    twin_route = [(i, i ^ 1) for i in range(devices)]
    ring = lax.ppermute(features, "strip", ring_route)
    twin = lax.ppermute(features, "strip", twin_route)
    fars = []
    start = 0
    for count in FAR_CHUNKS:
        piece = twin[start * width : (start + count) * width]
        fars.append(lax.ppermute(piece, "strip", far_route))
        start += count
    end = twin[start * width :]
    cuts = [0, columns // 2, 3 * columns // 4, columns]
    ends = [lax.ppermute(end[:, :, : cuts[1]], "strip", far_route)]
    for t, planes in enumerate(RELAY_PLANES, 1):
        piece = end[:, :, cuts[t] : cuts[t + 1]]
        hops = relay_hops(devices, *planes)
        relayed = [target for _, target in hops[2]]
        route = [pair for pair in far_route if pair[1] not in relayed]
        ends.append(lax.ppermute(piece, "strip", route))
        for hop in hops:
            piece = lax.ppermute(piece, "strip", hop)
        ends.append(piece)
    ring_twin = lax.ppermute(ring, "strip", twin_route)
    matrices = banded_matrices(row_kernel, odd, strip_rows)
    own = features
    part = mix(own, mix_weight, channel_bias)
    part = add_pair(matrices, own, OWN, twin, TWIN, part)
    part = add_pair(matrices, ring, RING, ring_twin, RING_TWIN, part)
    out = None
    start = 0
    for far, count in zip(fars, FAR_CHUNKS):
        out = finish(matrices, part, [far], out, start, count, None)
        start += count
    return finish(matrices, part, ends, out, start, 1, cuts)


def solution(mesh):
    return jax.shard_map(
        local,
        mesh=mesh,
        in_specs=(P(None, "strip", None), P(), P(), P()),
        out_specs=P(None, "strip", None),
        check_vma=False,
    )
```

```python
import functools

import jax
import jax.numpy as jnp
from jax import lax
from jax.experimental import pallas as pl
from jax.experimental.pallas import tpu as pltpu
from jax.sharding import PartitionSpec as P

FAR, RING_TWIN, OWN, TWIN, RING = range(5)
FAR_CHUNKS = (5, 2)
RELAYS = ((5, 1, False), (6, 2, True))
WHOLE = pl.BlockSpec(memory_space=pltpu.VMEM)
GRANT = pltpu.CompilerParams(vmem_limit_bytes=16 * 2**20)


def banded_kernel(odd_ref, rows_ref, out_ref):
    g = pl.program_id(0)
    roles, lanes = out_ref.shape[1:3]
    width = rows_ref.shape[2]
    rows = lanes // width
    shape = (rows, lanes)
    row = lax.broadcasted_iota(jnp.int32, shape, 0)
    column = lax.rem(lax.broadcasted_iota(jnp.int32, shape, 1), rows)
    keep = column >= row
    odd = odd_ref[0]
    for role in range(roles):
        place = jnp.where(odd == 1, roles - 1 - role, role)
        for o in range(width):
            now = jnp.broadcast_to(rows_ref[0, place + 1, o : o + 1, :], shape)
            before = jnp.broadcast_to(rows_ref[0, place, o : o + 1, :], shape)
            now = pltpu.roll(now, 0, 1, stride=1, stride_axis=0)
            before = pltpu.roll(before, lanes - rows, 1, stride=1, stride_axis=0)
            out_ref[g, role, o * rows : (o + 1) * rows, :] = jnp.where(keep, now, before).astype(
                jnp.bfloat16
            )


def banded_matrices(row_kernel, odd, strip_rows):
    groups, width, _, taps = row_kernel.shape
    places = (taps - 1) // strip_rows + 1
    padded = jnp.pad(
        row_kernel.astype(jnp.float32),
        ((0, 0), (0, 0), (0, 0), (strip_rows, places * strip_rows - taps)),
    )
    lanes = width * strip_rows
    rows = padded.reshape(groups, width, width, places + 1, strip_rows)
    rows = jnp.transpose(rows, (0, 3, 1, 2, 4)).reshape(groups, places + 1, width, lanes)
    return pl.pallas_call(
        banded_kernel,
        grid=(groups,),
        in_specs=[
            pl.BlockSpec(memory_space=pltpu.SMEM),
            pl.BlockSpec((1, places + 1, width, lanes), lambda g: (g, 0, 0, 0)),
        ],
        out_specs=WHOLE,
        out_shape=pltpu.VMEM((groups, places, lanes, lanes), jnp.bfloat16),
        compiler_params=GRANT,
        cost_estimate=pl.CostEstimate(flops=10**9, bytes_accessed=4 * 10**6, transcendentals=0),
        name="banded",
    )(odd, rows)


def mix_kernel(bias_ref, weight_ref, x_ref, out_ref, wide_ref):
    channels, part, columns = x_ref.shape
    size = channels * part

    @pl.when((pl.program_id(0) == 0) & (pl.program_id(1) == 0))
    def _():
        spread = lax.broadcasted_iota(jnp.int32, (size, channels), 0) // part
        spread = (spread == lax.broadcasted_iota(jnp.int32, (size, channels), 1)).astype(jnp.float32)
        spread = spread.astype(jnp.bfloat16)
        weight = weight_ref[...]
        tall = lax.dot_general(
            spread, weight, (((1,), (1,)), ((), ())), preferred_element_type=jnp.float32
        ).astype(jnp.bfloat16)
        wide = lax.dot_general(
            tall, spread, (((1,), (1,)), ((), ())), preferred_element_type=jnp.float32
        )
        row = lax.broadcasted_iota(jnp.int32, (size, size), 0) % part
        column = lax.broadcasted_iota(jnp.int32, (size, size), 1) % part
        wide_ref[...] = jnp.where(row == column, wide, 0.0).astype(jnp.bfloat16)

    x = x_ref[...].astype(jnp.float32).reshape(size, columns).astype(jnp.bfloat16)
    total = jnp.dot(wide_ref[...], x, preferred_element_type=jnp.float32)
    rows = pl.ds(pl.multiple_of(pl.program_id(0) * part, part), part)
    lanes = pl.ds(pl.multiple_of(pl.program_id(1) * columns, columns), columns)
    for c in range(channels):
        out_ref[c, rows, lanes] = total[c * part : (c + 1) * part] + bias_ref[c]


def mix(features, mix_weight, channel_bias):
    channels, rows, columns = features.shape
    part = 8
    half = columns // 2
    block = pl.BlockSpec((channels, part, half), lambda t, h: (0, t, h))
    return pl.pallas_call(
        mix_kernel,
        grid=(rows // part, 2),
        in_specs=[
            pl.BlockSpec(memory_space=pltpu.SMEM),
            pl.BlockSpec((channels, channels), lambda t, h: (0, 0)),
            block,
        ],
        out_specs=WHOLE,
        out_shape=pltpu.VMEM(features.shape, jnp.float32),
        compiler_params=GRANT,
        scratch_shapes=[pltpu.VMEM((channels * part, channels * part), jnp.bfloat16)],
        cost_estimate=pl.CostEstimate(
            flops=2 * part * channels * features.size,
            bytes_accessed=6 * features.size,
            transcendentals=0,
        ),
        name="mix",
    )(channel_bias, mix_weight, features)


def pair_kernel(first_role, second_role, matrix_ref, first_ref, second_ref, part_ref, out_ref):
    g = pl.program_id(0)
    width, rows, columns = first_ref.shape
    flat = (width * rows, columns)
    total = jnp.dot(
        matrix_ref[g, first_role], first_ref[...].reshape(flat), preferred_element_type=jnp.float32
    )
    total += jnp.dot(
        matrix_ref[g, second_role], second_ref[...].reshape(flat), preferred_element_type=jnp.float32
    )
    here = pl.ds(g * width, width)
    out_ref[here] = part_ref[here] + total.reshape(width, rows, columns)


def add_pair(matrices, first, first_role, second, second_role, part):
    groups, _, lanes, _ = matrices.shape
    channels, rows, columns = first.shape
    width = channels // groups
    strip = pl.BlockSpec((width, rows, columns), lambda g: (g, 0, 0))
    return pl.pallas_call(
        functools.partial(pair_kernel, first_role, second_role),
        grid=(groups,),
        in_specs=[WHOLE, strip, strip, WHOLE],
        out_specs=WHOLE,
        out_shape=pltpu.VMEM(part.shape, jnp.float32),
        input_output_aliases={3: 0},
        compiler_params=GRANT,
        cost_estimate=pl.CostEstimate(
            flops=4 * lanes * first.size, bytes_accessed=4 * first.size, transcendentals=0
        ),
    )(matrices, first, second, part)


def last_kernel(start, count, cuts, matrix_ref, part_ref, *refs):
    out_ref, ready_ref, sems = refs[-3:]
    width = ready_ref.shape[0] // count
    rows, columns = ready_ref.shape[1:]
    edges = [0, columns // 2, columns] if cuts is None else cuts
    tiles = list(zip(edges, edges[1:]))

    def far(g, t):
        lanes = slice(*tiles[t])
        if cuts is None:
            return refs[0][pl.ds(g * width, width), :, lanes]
        if t == 0:
            return refs[0][...]
        return refs[2 * t - 1][...] + refs[2 * t][...]

    def copy(g, t):
        lanes = pl.ds(tiles[t][0], tiles[t][1] - tiles[t][0])
        return pltpu.make_async_copy(
            ready_ref.at[pl.ds(g * width, width), :, lanes],
            out_ref.at[pl.ds((start + g) * width, width), :, lanes],
            sems.at[len(tiles) * g + t],
        )

    def group(g):
        for t, (first, last) in enumerate(tiles):
            lanes = slice(first, last)
            total = jnp.dot(
                matrix_ref[start + g, FAR],
                far(g, t).reshape(width * rows, last - first),
                preferred_element_type=jnp.float32,
            )
            total = part_ref[pl.ds((start + g) * width, width), :, lanes] + total.reshape(
                width, rows, last - first
            )
            ready_ref[pl.ds(g * width, width), :, lanes] = jax.nn.gelu(total).astype(jnp.bfloat16)
            copy(g, t).start()

    if count == 1:
        group(0)
    else:
        pl.loop(0, count)(group)
    for g in range(count):
        for t in range(len(tiles)):
            copy(g, t).wait()


def finish(matrices, part, fars, out, start, count, cuts):
    groups, _, lanes, _ = matrices.shape
    channels, rows, columns = part.shape
    width = channels // groups
    given = [] if out is None else [out]
    whole = pl.BlockSpec(memory_space=pl.ANY)
    size = count * width * rows * columns
    return pl.pallas_call(
        functools.partial(last_kernel, start, count, cuts),
        in_specs=[WHOLE] * (2 + len(fars)) + [whole] * len(given),
        out_specs=whole,
        out_shape=jax.ShapeDtypeStruct(part.shape, jnp.bfloat16),
        input_output_aliases={2 + len(fars): 0} if given else {},
        scratch_shapes=[
            pltpu.VMEM((count * width, rows, columns), jnp.bfloat16),
            pltpu.SemaphoreType.DMA((3 * count,)),
        ],
        compiler_params=GRANT,
        cost_estimate=pl.CostEstimate(
            flops=2 * lanes * size, bytes_accessed=4 * size, transcendentals=size
        ),
    )(matrices, part, *fars, *given)


def relay_hops(devices, up_plane, down_plane, inner):
    if devices != 256:
        return [], [], []

    def strip(x, z, y, core):
        return ((x % 4 * 8 + z % 8) * 4 + y) * 2 + core

    paths = []
    for x in range(4):
        low, high = strip(x - 1, 7, 3, 1), strip(x, 0, 0, 0)
        paths.append([low, strip(x - 1, up_plane, 3, 1), strip(x, up_plane, 0, 1), high])
        paths.append([high, strip(x, down_plane, 0, 1), strip(x - 1, down_plane, 3, 1), low])
        for z in range(1, 8) if inner else ():
            low, high = strip(x, z - 1, 3, 1), strip(x, z, 0, 0)
            paths.append([low, strip(x, z - 1, 2, 1), strip(x, z - 1, 1, 1), high])
            paths.append([high, strip(x, z, 1, 0), strip(x, z, 2, 0), low])
    return tuple([tuple(path[i : i + 2]) for path in paths] for i in range(3))


def local(features, row_kernel, mix_weight, channel_bias):
    strip_rows, columns = features.shape[1:]
    width = row_kernel.shape[1]
    devices = lax.axis_size("strip")
    odd = lax.rem(lax.axis_index("strip"), 2).reshape(1)
    ring_route = [(i, (i + (2 if i % 2 else -2)) % devices) for i in range(devices)]
    far_route = [(i, (i + (1 if i % 2 else -1)) % devices) for i in range(devices)]
    twin_route = [(i, i ^ 1) for i in range(devices)]
    ring = lax.ppermute(features, "strip", ring_route)
    twin = lax.ppermute(features, "strip", twin_route)
    fars = []
    start = 0
    for count in FAR_CHUNKS:
        piece = twin[start * width : (start + count) * width]
        fars.append(lax.ppermute(piece, "strip", far_route))
        start += count
    end = twin[start * width :]
    cuts = [0, 3 * columns // 8, 3 * columns // 4, columns]
    ends = [lax.ppermute(end[:, :, : cuts[1]], "strip", far_route)]
    for t, relay in enumerate(RELAYS, 1):
        piece = end[:, :, cuts[t] : cuts[t + 1]]
        hops = relay_hops(devices, *relay)
        relayed = [target for _, target in hops[2]]
        route = [pair for pair in far_route if pair[1] not in relayed]
        ends.append(lax.ppermute(piece, "strip", route))
        for hop in hops:
            piece = lax.ppermute(piece, "strip", hop)
        ends.append(piece)
    ring_twin = lax.ppermute(ring, "strip", twin_route)
    matrices = banded_matrices(row_kernel, odd, strip_rows)
    own = features
    part = mix(own, mix_weight, channel_bias)
    part = add_pair(matrices, own, OWN, twin, TWIN, part)
    part = add_pair(matrices, ring, RING, ring_twin, RING_TWIN, part)
    out = None
    start = 0
    for far, count in zip(fars, FAR_CHUNKS):
        out = finish(matrices, part, [far], out, start, count, None)
        start += count
    return finish(matrices, part, ends, out, start, 1, cuts)


def solution(mesh):
    return jax.shard_map(
        local,
        mesh=mesh,
        in_specs=(P(None, "strip", None), P(), P(), P()),
        out_specs=P(None, "strip", None),
        check_vma=False,
    )
```

```python
import functools

import jax
import jax.numpy as jnp
from jax import lax
from jax.experimental import pallas as pl
from jax.experimental.pallas import tpu as pltpu
from jax.sharding import PartitionSpec as P

FAR, RING_TWIN, OWN, TWIN, RING = range(5)
FAR_CHUNKS = (6, 1)
RELAYS = ((5, 1, False), (6, 2, True))
WHOLE = pl.BlockSpec(memory_space=pltpu.VMEM)
GRANT = pltpu.CompilerParams(vmem_limit_bytes=16 * 2**20)


def banded_kernel(odd_ref, rows_ref, out_ref):
    g = pl.program_id(0)
    roles, lanes = out_ref.shape[1:3]
    width = rows_ref.shape[2]
    rows = lanes // width
    shape = (rows, lanes)
    row = lax.broadcasted_iota(jnp.int32, shape, 0)
    column = lax.rem(lax.broadcasted_iota(jnp.int32, shape, 1), rows)
    keep = column >= row
    odd = odd_ref[0]
    for role in range(roles):
        place = jnp.where(odd == 1, roles - 1 - role, role)
        for o in range(width):
            now = jnp.broadcast_to(rows_ref[0, place + 1, o : o + 1, :], shape)
            before = jnp.broadcast_to(rows_ref[0, place, o : o + 1, :], shape)
            now = pltpu.roll(now, 0, 1, stride=1, stride_axis=0)
            before = pltpu.roll(before, lanes - rows, 1, stride=1, stride_axis=0)
            out_ref[g, role, o * rows : (o + 1) * rows, :] = jnp.where(keep, now, before).astype(
                jnp.bfloat16
            )


def banded_matrices(row_kernel, odd, strip_rows):
    groups, width, _, taps = row_kernel.shape
    places = (taps - 1) // strip_rows + 1
    padded = jnp.pad(
        row_kernel.astype(jnp.float32),
        ((0, 0), (0, 0), (0, 0), (strip_rows, places * strip_rows - taps)),
    )
    lanes = width * strip_rows
    rows = padded.reshape(groups, width, width, places + 1, strip_rows)
    rows = jnp.transpose(rows, (0, 3, 1, 2, 4)).reshape(groups, places + 1, width, lanes)
    return pl.pallas_call(
        banded_kernel,
        grid=(groups,),
        in_specs=[
            pl.BlockSpec(memory_space=pltpu.SMEM),
            pl.BlockSpec((1, places + 1, width, lanes), lambda g: (g, 0, 0, 0)),
        ],
        out_specs=WHOLE,
        out_shape=pltpu.VMEM((groups, places, lanes, lanes), jnp.bfloat16),
        compiler_params=GRANT,
        cost_estimate=pl.CostEstimate(flops=10**9, bytes_accessed=4 * 10**6, transcendentals=0),
        name="banded",
    )(odd, rows)


def mix_kernel(bias_ref, weight_ref, x_ref, out_ref, wide_ref):
    channels, part, columns = x_ref.shape
    size = channels * part

    @pl.when((pl.program_id(0) == 0) & (pl.program_id(1) == 0))
    def _():
        spread = lax.broadcasted_iota(jnp.int32, (size, channels), 0) // part
        spread = (spread == lax.broadcasted_iota(jnp.int32, (size, channels), 1)).astype(jnp.float32)
        spread = spread.astype(jnp.bfloat16)
        weight = weight_ref[...]
        tall = lax.dot_general(
            spread, weight, (((1,), (1,)), ((), ())), preferred_element_type=jnp.float32
        ).astype(jnp.bfloat16)
        wide = lax.dot_general(
            tall, spread, (((1,), (1,)), ((), ())), preferred_element_type=jnp.float32
        )
        row = lax.broadcasted_iota(jnp.int32, (size, size), 0) % part
        column = lax.broadcasted_iota(jnp.int32, (size, size), 1) % part
        wide_ref[...] = jnp.where(row == column, wide, 0.0).astype(jnp.bfloat16)

    x = x_ref[...].astype(jnp.float32).reshape(size, columns).astype(jnp.bfloat16)
    total = jnp.dot(wide_ref[...], x, preferred_element_type=jnp.float32)
    rows = pl.ds(pl.multiple_of(pl.program_id(0) * part, part), part)
    lanes = pl.ds(pl.multiple_of(pl.program_id(1) * columns, columns), columns)
    for c in range(channels):
        out_ref[c, rows, lanes] = total[c * part : (c + 1) * part] + bias_ref[c]


def mix(features, mix_weight, channel_bias):
    channels, rows, columns = features.shape
    part = 8
    half = columns // 2
    block = pl.BlockSpec((channels, part, half), lambda t, h: (0, t, h))
    return pl.pallas_call(
        mix_kernel,
        grid=(rows // part, 2),
        in_specs=[
            pl.BlockSpec(memory_space=pltpu.SMEM),
            pl.BlockSpec((channels, channels), lambda t, h: (0, 0)),
            block,
        ],
        out_specs=WHOLE,
        out_shape=pltpu.VMEM(features.shape, jnp.float32),
        compiler_params=GRANT,
        scratch_shapes=[pltpu.VMEM((channels * part, channels * part), jnp.bfloat16)],
        cost_estimate=pl.CostEstimate(
            flops=2 * part * channels * features.size,
            bytes_accessed=6 * features.size,
            transcendentals=0,
        ),
        name="mix",
    )(channel_bias, mix_weight, features)


def pair_kernel(first_role, second_role, matrix_ref, first_ref, second_ref, part_ref, out_ref):
    g = pl.program_id(0)
    width, rows, columns = first_ref.shape
    flat = (width * rows, columns)
    total = jnp.dot(
        matrix_ref[g, first_role], first_ref[...].reshape(flat), preferred_element_type=jnp.float32
    )
    total += jnp.dot(
        matrix_ref[g, second_role], second_ref[...].reshape(flat), preferred_element_type=jnp.float32
    )
    here = pl.ds(g * width, width)
    out_ref[here] = part_ref[here] + total.reshape(width, rows, columns)


def add_pair(matrices, first, first_role, second, second_role, part):
    groups, _, lanes, _ = matrices.shape
    channels, rows, columns = first.shape
    width = channels // groups
    strip = pl.BlockSpec((width, rows, columns), lambda g: (g, 0, 0))
    return pl.pallas_call(
        functools.partial(pair_kernel, first_role, second_role),
        grid=(groups,),
        in_specs=[WHOLE, strip, strip, WHOLE],
        out_specs=WHOLE,
        out_shape=pltpu.VMEM(part.shape, jnp.float32),
        input_output_aliases={3: 0},
        compiler_params=GRANT,
        cost_estimate=pl.CostEstimate(
            flops=4 * lanes * first.size, bytes_accessed=4 * first.size, transcendentals=0
        ),
    )(matrices, first, second, part)


def last_kernel(start, count, tiles, matrix_ref, part_ref, *refs):
    out_ref, ready_ref, sems = refs[-3:]
    width = ready_ref.shape[0] // count
    rows = ready_ref.shape[1]

    def copy(g, t):
        first, last, _ = tiles[t]
        lanes = pl.ds(first, last - first)
        return pltpu.make_async_copy(
            ready_ref.at[pl.ds(g * width, width), :, lanes],
            out_ref.at[pl.ds((start + g) * width, width), :, lanes],
            sems.at[len(tiles) * g + t],
        )

    def group(g):
        here = pl.ds(g * width, width)
        for t, (first, last, sources) in enumerate(tiles):
            far = [refs[i][here, :, first - at : last - at] for i, at in sources]
            far = far[0] if len(far) == 1 else far[0] + far[1]
            total = jnp.dot(
                matrix_ref[start + g, FAR],
                far.reshape(width * rows, last - first),
                preferred_element_type=jnp.float32,
            )
            total = part_ref[pl.ds((start + g) * width, width), :, first:last] + total.reshape(
                width, rows, last - first
            )
            ready_ref[here, :, first:last] = jax.nn.gelu(total).astype(jnp.bfloat16)
            copy(g, t).start()

    if count == 1:
        group(0)
    else:
        pl.loop(0, count)(group)
    for g in range(count):
        for t in range(len(tiles)):
            copy(g, t).wait()


def finish(matrices, part, fars, out, start, count, tiles):
    groups, _, lanes, _ = matrices.shape
    channels, rows, columns = part.shape
    width = channels // groups
    given = [] if out is None else [out]
    whole = pl.BlockSpec(memory_space=pl.ANY)
    size = count * width * rows * sum(last - first for first, last, _ in tiles)
    return pl.pallas_call(
        functools.partial(last_kernel, start, count, tiles),
        in_specs=[WHOLE] * (2 + len(fars)) + [whole] * len(given),
        out_specs=whole,
        out_shape=jax.ShapeDtypeStruct(part.shape, jnp.bfloat16),
        input_output_aliases={2 + len(fars): 0} if given else {},
        scratch_shapes=[
            pltpu.VMEM((count * width, rows, columns), jnp.bfloat16),
            pltpu.SemaphoreType.DMA((len(tiles) * count,)),
        ],
        compiler_params=GRANT,
        cost_estimate=pl.CostEstimate(
            flops=2 * lanes * size, bytes_accessed=4 * size, transcendentals=size
        ),
    )(matrices, part, *fars, *given)


def relay_hops(devices, up_plane, down_plane, inner):
    if devices != 256:
        return [], [], []

    def strip(x, z, y, core):
        return ((x % 4 * 8 + z % 8) * 4 + y) * 2 + core

    paths = []
    for x in range(4):
        low, high = strip(x - 1, 7, 3, 1), strip(x, 0, 0, 0)
        paths.append([low, strip(x - 1, up_plane, 3, 1), strip(x, up_plane, 0, 1), high])
        paths.append([high, strip(x, down_plane, 0, 1), strip(x - 1, down_plane, 3, 1), low])
        for z in range(1, 8) if inner else ():
            low, high = strip(x, z - 1, 3, 1), strip(x, z, 0, 0)
            if z in (RELAYS[0][0], up_plane):
                paths.append([low, strip(x, z - 1, 2, 1), strip(x, z - 1, 1, 1), high])
            paths.append([high, strip(x, z, 1, 0), strip(x, z, 2, 0), low])
    if not inner:
        paths.append([strip(0, 0, 1, 0), strip(1, 0, 1, 1), strip(1, 0, 0, 1), strip(0, 0, 0, 1)])
    return tuple([tuple(path[i : i + 2]) for path in paths] for i in range(3))


def local(features, row_kernel, mix_weight, channel_bias):
    strip_rows, columns = features.shape[1:]
    width = row_kernel.shape[1]
    devices = lax.axis_size("strip")
    odd = lax.rem(lax.axis_index("strip"), 2).reshape(1)
    ring_route = [(i, (i + (2 if i % 2 else -2)) % devices) for i in range(devices)]
    far_route = [(i, (i + (1 if i % 2 else -1)) % devices) for i in range(devices)]
    twin_route = [(i, i ^ 1) for i in range(devices)]
    ring = lax.ppermute(features, "strip", ring_route)
    twin = lax.ppermute(features, "strip", twin_route)
    fars = []
    start = 0
    for count in FAR_CHUNKS:
        piece = twin[start * width : (start + count) * width]
        fars.append(lax.ppermute(piece, "strip", far_route))
        start += count
    end = twin[start * width :]
    cuts = [0, 3 * columns // 8, 3 * columns // 4, columns]
    ends = []
    for t, relay in enumerate(RELAYS):
        piece = end[:, :, cuts[t] : cuts[t + 1]]
        hops = relay_hops(devices, *relay)
        relayed = [target for _, target in hops[2]]
        route = [pair for pair in far_route if pair[1] not in relayed]
        ends.append(lax.ppermute(piece, "strip", route))
        for hop in hops:
            piece = lax.ppermute(piece, "strip", hop)
        ends.append(piece)
    final = lax.ppermute(end[:, :, cuts[2] :], "strip", far_route)
    ring_twin = lax.ppermute(ring, "strip", twin_route)
    matrices = banded_matrices(row_kernel, odd, strip_rows)
    own = features
    part = mix(own, mix_weight, channel_bias)
    part = add_pair(matrices, own, OWN, twin, TWIN, part)
    part = add_pair(matrices, ring, RING, ring_twin, RING_TWIN, part)
    half = columns // 2
    all_columns = ((0, half, ((0, 0),)), (half, columns, ((0, 0),)))
    relayed_columns = (
        (cuts[0], cuts[1], ((0, cuts[0]), (1, cuts[0]))),
        (cuts[1], cuts[2], ((2, cuts[1]), (3, cuts[1]))),
    )
    edge = 7 * columns // 8
    final_columns = ((cuts[2], edge, ((0, cuts[2]),)), (edge, columns, ((0, cuts[2]),)))
    first, second = FAR_CHUNKS
    out = finish(matrices, part, fars[:1], None, 0, first, all_columns)
    out = finish(matrices, part, ends, out, first + second, 1, relayed_columns)
    out = finish(matrices, part, fars[1:], out, first, second, all_columns)
    return finish(matrices, part, [final], out, first + second, 1, final_columns)


def solution(mesh):
    return jax.shard_map(
        local,
        mesh=mesh,
        in_specs=(P(None, "strip", None), P(), P(), P()),
        out_specs=P(None, "strip", None),
        check_vma=False,
    )
```
